32 devices in a mesh: blk: 16 (over z, x, core), feat: 2 (over y).
Axes of the slice: x: 2, y: 2, z: 4, core: 2. Of those that a mesh axis runs over, the one named last changes fastest.
Arguments:
- samples: float32 [12288, 2048], P('blk', 'feat'), may hold values from -6 to 6
Outputs:
- band: float32 [5, 12288, 768], P(None, 'blk', 'feat')
The draws below stay inside these ranges and needn't reach their ends.
All inputs are finite; a program needn't handle non-finite values.
Results may differ from the reference program's by a relative error of at most 0.0001.
Values sent between devices are 32-bit elements; how exact they have to be, the bound alone decides.
A program may use at most 128 MiB of HBM per device.

```python
import jax
import jax.numpy as jnp
from jax import lax

F = 2048
S_DEV = 768
HALF = 2
SAMPLES = 12288


def shard_levels(key, extent, pieces, low, top_value):
    gain, own = 1.0, jax.random.fold_in(key, 6)
    for position, blocks in pieces:
        heights = jnp.exp(jax.random.uniform(jax.random.fold_in(own, position), (blocks,), jnp.float32, low / len(pieces), top_value / len(pieces)))
        gain = gain * jnp.repeat(heights, extent[position] // blocks).reshape([-1 if axis == position else 1 for axis in range(len(extent))])
    return gain


def gaussian(key, shape, width, reach, shards=(), kind=jnp.bfloat16):
    factor_of = shard_levels(key, shape, shards, -0.22, 0.18) if shards else 1.0
    values = jax.random.normal(key, shape, jnp.float32) * width * factor_of
    return jnp.minimum(jnp.maximum(values, -reach), reach).astype(kind)


def setup_inputs(seed: int = 0) -> dict:
    streams_of = jax.random.split(jax.random.key(seed), 2)
    samples = gaussian(streams_of[0], (SAMPLES, F), 1.0, 6.0, ((0, 16), (1, 2)), jnp.float32)
    return {"samples": samples}


def reference(samples):
    blocks = samples.reshape(-1, S_DEV, F)
    scale = 1.0 / jnp.sqrt(jnp.float32(F))
    results = []
    for index in range(2 * HALF + 1):
        other = jnp.roll(blocks, -(index - HALF), axis=0)
        prod = jnp.einsum('isf,itf->ist', blocks, other, precision=lax.Precision.HIGHEST, preferred_element_type=jnp.float32)
        results.append((prod * scale).reshape(-1, S_DEV))
    return jnp.stack(results)
```

```python
import functools

import jax
import jax.numpy as jnp
from jax import lax
from jax.experimental import pallas as pl
from jax.experimental.pallas import tpu as pltpu
from jax.sharding import PartitionSpec as P

MESH = pl.DeviceIdType.MESH
CHUNK = 128
AHEAD = 3
RING = 3
Y, X, Z, C, R = range(5)


def left_split(value):
    high = value.astype(jnp.bfloat16)
    low = (value - high.astype(jnp.float32)).astype(jnp.bfloat16)
    return jnp.concatenate([high, high, low], axis=1)


def right_split(value):
    high = value.astype(jnp.bfloat16)
    low = (value - high.astype(jnp.float32)).astype(jnp.bfloat16)
    return jnp.concatenate([high, low, high], axis=1)


def kernel(n, scale, x_hbm, o_hbm, own, bx, bz, bc, br, acc, left, send, recv, local, outs):
    rows = x_hbm.shape[0]
    half = rows // 2
    kl = x_hbm.shape[1] // CHUNK
    steps = 2 * kl
    b, f = lax.axis_index("blk"), lax.axis_index("feat")
    core = lax.rem(b, 2)
    group = lax.rem(b // 2, 2)
    near = b + 2 - 4 * group
    onward = lax.rem(b + jnp.where(group == 0, 4, n - 4), n)
    source = lax.rem(b + jnp.where(group == 0, n - 4, 4), n)
    mate = b + 1 - 2 * core
    gives_x = core == group

    def mine(k, h):
        start = pl.multiple_of(jnp.where(h == 0, f, 1 - f) * half, half)
        column = pl.multiple_of(k * CHUNK, CHUNK)
        return pltpu.make_async_copy(
            x_hbm.at[pl.ds(start, half), pl.ds(column, CHUNK)], own.at[k, h], local.at[h, k]
        )

    def remote(kind, k, src, dst, target):
        return pltpu.make_async_remote_copy(
            src_ref=src,
            dst_ref=dst,
            send_sem=send.at[kind, k],
            recv_sem=recv.at[kind, k],
            device_id=target,
            device_id_type=MESH,
        )

    def y_copy(t):
        k, phase = lax.rem(t, kl), t // kl
        return remote(Y, t, own.at[k, 1 - phase], own.at[kl + k, phase], (b, 1 - f))

    def x_copy(k):
        return remote(X, k, own.at[k, 0], bx.at[k], (near, f))

    def z_copy(k):
        return remote(Z, k, bx.at[k], bz.at[k], (onward, f))

    def c_copy(k):
        return remote(C, k, own.at[k, 0], bc.at[k], (mate, f))

    def r_copy(k, src):
        return remote(R, k, src.at[k], br.at[k], (mate, f))

    def load(k, _):
        mine(k, 0).start()
        mine(k, 1).start()
        return 0

    lax.fori_loop(0, kl, load, 0)
    barrier = pltpu.get_barrier_semaphore()
    for device in ((b, 1 - f), (near, f), (mate, f), (onward, f), (source, f)):
        pl.semaphore_signal(barrier, inc=1, device_id=device, device_id_type=MESH)
    pl.semaphore_wait(barrier, 5)

    def begin(k, _):
        mine(k, 0).wait()
        mine(k, 1).wait()

        @pl.when(k < AHEAD)
        def _():
            x_copy(k).start()
            y_copy(k).start()

        c_copy(k).start()
        return 0

    lax.fori_loop(0, kl, begin, 0)
    acc[...] = jnp.zeros_like(acc)

    def add(j, k, block):
        acc[j] += lax.dot_general(
            left[lax.rem(k, RING)],
            right_split(block),
            (((1,), (1,)), ((), ())),
            preferred_element_type=jnp.float32,
        )

    def step(t, _):
        @pl.when(t < steps)
        def _():
            y_copy(t).wait_recv()

            @pl.when(t < kl)
            def _():
                c_copy(kl + t).start()

            @pl.when(t + AHEAD < steps)
            def _():
                x_copy(t + AHEAD).start()
                y_copy(t + AHEAD).start()

            x_copy(t).wait_recv()
            z_copy(t).start()

            @pl.when(gives_x)
            def _():
                r_copy(t, bx).start()

        @pl.when(jnp.logical_and(t >= 1, t <= steps))
        def _():
            z_copy(t - 1).wait_recv()

            @pl.when(jnp.logical_not(gives_x))
            def _():
                r_copy(t - 1, bz).start()

        @pl.when(t < steps)
        def _():
            c_copy(t).wait_recv()
            whole = own[t].reshape(rows, CHUNK)
            left[lax.rem(t, RING)] = left_split(whole * scale)
            add(0, t, own[t, 0])
            add(1, t, bc[t])
            add(2, t, bx[t])

        @pl.when(jnp.logical_and(t >= 1, t <= steps))
        def _():
            add(3, t - 1, bz[t - 1])

        @pl.when(t >= 2)
        def _():
            r_copy(t - 2, bx).wait_recv()
            add(4, t - 2, br[t - 2])

        return 0

    lax.fori_loop(0, steps + 2, step, 0)

    slots = (2, 3 - 2 * core, 4 - 4 * group, 4 * group, 1 + 2 * core)

    def out(j, h):
        start = pl.multiple_of((f if h == 0 else 1 - f) * half, half)
        return pltpu.make_async_copy(
            acc.at[j, pl.ds(h * half, half)], o_hbm.at[slots[j], pl.ds(start, half)], outs.at[j, h]
        )

    for j in range(5):
        for h in range(2):
            out(j, h).start()

    def drain(k, _):
        y_copy(k).wait_send()
        x_copy(k).wait_send()
        z_copy(k).wait_send()
        c_copy(k).wait_send()
        r_copy(k, bx).wait_send()
        return 0

    lax.fori_loop(0, steps, drain, 0)
    for j in range(5):
        for h in range(2):
            out(j, h).wait()


def solution(mesh):
    n = mesh.shape["blk"]

    def local(samples):
        rows, width = samples.shape
        half = rows // 2
        steps = 2 * width // CHUNK
        block = pltpu.VMEM((steps, half, CHUNK), jnp.float32)
        scale = 1.0 / float(width * mesh.shape["feat"]) ** 0.5
        return pl.pallas_call(
            functools.partial(kernel, n, scale),
            out_shape=jax.ShapeDtypeStruct((5, rows, half), jnp.float32),
            in_specs=[pl.BlockSpec(memory_space=pl.ANY)],
            out_specs=pl.BlockSpec(memory_space=pl.ANY),
            scratch_shapes=[
                pltpu.VMEM((steps, 2, half, CHUNK), jnp.float32),
                block,
                block,
                block,
                block,
                pltpu.VMEM((5, rows, half), jnp.float32),
                pltpu.VMEM((RING, rows, 3 * CHUNK), jnp.bfloat16),
                pltpu.SemaphoreType.DMA((5, steps)),
                pltpu.SemaphoreType.DMA((5, steps)),
                pltpu.SemaphoreType.DMA((2, steps // 2)),
                pltpu.SemaphoreType.DMA((5, 2)),
            ],
            compiler_params=pltpu.CompilerParams(
                collective_id=0, has_side_effects=True, vmem_limit_bytes=60 << 20
            ),
            name="band",
        )(samples)

    return jax.shard_map(
        local, mesh=mesh, in_specs=(P("blk", "feat"),), out_specs=P(None, "blk", "feat"), check_vma=False
    )
```

```python
import functools

import jax
import jax.numpy as jnp
from jax import lax
from jax.experimental import pallas as pl
from jax.experimental.pallas import tpu as pltpu
from jax.sharding import PartitionSpec as P

MESH = pl.DeviceIdType.MESH
CHUNK = 128
PARTS = 1
AHEAD = 3
RING = 3
Y, C, R = range(3)


def left_split(value):
    high = value.astype(jnp.bfloat16)
    low = (value - high.astype(jnp.float32)).astype(jnp.bfloat16)
    return jnp.concatenate([high, high, low], axis=1)


def right_split(value):
    high = value.astype(jnp.bfloat16)
    low = (value - high.astype(jnp.float32)).astype(jnp.bfloat16)
    return jnp.concatenate([high, low, high], axis=1)


def kernel(n, scale, x_hbm, acc, own, bx, bz, bc, br, left, send, recv, sendx, recvx, sendz, recvz, local):
    rows = x_hbm.shape[0]
    half = rows // 2
    kl = x_hbm.shape[1] // CHUNK
    steps = 2 * kl
    b, f = lax.axis_index("blk"), lax.axis_index("feat")
    core = lax.rem(b, 2)
    group = lax.rem(b // 2, 2)
    near = b + 2 - 4 * group
    onward = lax.rem(b + jnp.where(group == 0, 4, n - 4), n)
    source = lax.rem(b + jnp.where(group == 0, n - 4, 4), n)
    mate = b + 1 - 2 * core
    gives_x = core == group

    def mine(k, h):
        start = pl.multiple_of(jnp.where(h == 0, f, 1 - f) * half, half)
        column = pl.multiple_of(k * CHUNK, CHUNK)
        return pltpu.make_async_copy(
            x_hbm.at[pl.ds(start, half), pl.ds(column, CHUNK)], own.at[k, h], local.at[h, k]
        )

    def remote(kind, k, src, dst, target):
        return pltpu.make_async_remote_copy(
            src_ref=src,
            dst_ref=dst,
            send_sem=send.at[kind, k],
            recv_sem=recv.at[kind, k],
            device_id=target,
            device_id_type=MESH,
        )

    def y_copy(t):
        k, phase = lax.rem(t, kl), t // kl
        return remote(Y, t, own.at[k, 1 - phase], own.at[kl + k, phase], (b, 1 - f))

    def part(s):
        return pl.ds(s * (half // PARTS), half // PARTS)

    def x_copy(k, s):
        return pltpu.make_async_remote_copy(
            src_ref=own.at[k, 0, part(s)],
            dst_ref=bx.at[k, part(s)],
            send_sem=sendx.at[s, k],
            recv_sem=recvx.at[s, k],
            device_id=(near, f),
            device_id_type=MESH,
        )

    def z_copy(k, s):
        return pltpu.make_async_remote_copy(
            src_ref=bx.at[k, part(s)],
            dst_ref=bz.at[k, part(s)],
            send_sem=sendz.at[s, k],
            recv_sem=recvz.at[s, k],
            device_id=(onward, f),
            device_id_type=MESH,
        )

    def c_copy(k):
        return remote(C, k, own.at[k, 0], bc.at[k], (mate, f))

    def r_copy(k, src):
        return remote(R, k, src.at[k], br.at[k], (mate, f))

    def load(k, _):
        mine(k, 0).start()
        mine(k, 1).start()
        return 0

    lax.fori_loop(0, kl, load, 0)
    barrier = pltpu.get_barrier_semaphore()
    for device in ((b, 1 - f), (near, f), (mate, f), (onward, f), (source, f)):
        pl.semaphore_signal(barrier, inc=1, device_id=device, device_id_type=MESH)
    pl.semaphore_wait(barrier, 5)

    def begin(k, _):
        mine(k, 0).wait()
        mine(k, 1).wait()

        @pl.when(k < AHEAD)
        def _():
            for s in range(PARTS):
                x_copy(k, s).start()
            y_copy(k).start()

        c_copy(k).start()
        return 0

    lax.fori_loop(0, kl, begin, 0)
    acc[...] = jnp.zeros_like(acc)

    slots = (2, 3 - 2 * core, 4 - 4 * group, 4 * group, 1 + 2 * core)

    def add(j, k, block):
        right = right_split(block)
        for h in range(2):
            start = pl.multiple_of((f if h == 0 else 1 - f) * half, half)
            acc[slots[j], pl.ds(start, half)] += lax.dot_general(
                left[lax.rem(k, RING), h],
                right,
                (((1,), (1,)), ((), ())),
                preferred_element_type=jnp.float32,
            )

    def step(t, _):
        for s in range(PARTS):

            @pl.when(t < steps)
            def _():
                if s == 0:
                    y_copy(t).wait_recv()

                    @pl.when(t < kl)
                    def _():
                        c_copy(kl + t).start()

                    @pl.when(t + AHEAD < steps)
                    def _():
                        for r in range(PARTS):
                            x_copy(t + AHEAD, r).start()
                        y_copy(t + AHEAD).start()

                x_copy(t, s).wait_recv()
                z_copy(t, s).start()

                if s == PARTS - 1:

                    @pl.when(gives_x)
                    def _():
                        r_copy(t, bx).start()

                if s == 0:
                    for h in range(2):
                        left[lax.rem(t, RING), h] = left_split(own[t, h] * scale)
                    add(0, t, own[t, 0])
                if s == PARTS - 1:
                    c_copy(t).wait_recv()
                    add(1, t, bc[t])

            if s == 0:

                @pl.when(jnp.logical_and(t >= 1, t <= steps))
                def _():
                    for r in range(PARTS):
                        z_copy(t - 1, r).wait_recv()

                    @pl.when(jnp.logical_not(gives_x))
                    def _():
                        r_copy(t - 1, bz).start()

                    add(3, t - 1, bz[t - 1])

        @pl.when(t < steps)
        def _():
            add(2, t, bx[t])

        @pl.when(t >= 2)
        def _():
            r_copy(t - 2, bx).wait_recv()
            add(4, t - 2, br[t - 2])

        return 0

    lax.fori_loop(0, steps + 2, step, 0)

    def drain(k, _):
        y_copy(k).wait_send()
        for s in range(PARTS):
            x_copy(k, s).wait_send()
            z_copy(k, s).wait_send()
        c_copy(k).wait_send()
        r_copy(k, bx).wait_send()
        return 0

    lax.fori_loop(0, steps, drain, 0)


def solution(mesh):
    n = mesh.shape["blk"]

    def local(samples):
        rows, width = samples.shape
        half = rows // 2
        steps = 2 * width // CHUNK
        block = pltpu.VMEM((steps, half, CHUNK), jnp.float32)
        scale = 1.0 / float(width * mesh.shape["feat"]) ** 0.5
        return pl.pallas_call(
            functools.partial(kernel, n, scale),
            out_shape=pltpu.VMEM((5, rows, half), jnp.float32),
            in_specs=[pl.BlockSpec(memory_space=pl.ANY)],
            out_specs=pl.BlockSpec(memory_space=pltpu.VMEM),
            scratch_shapes=[
                pltpu.VMEM((steps, 2, half, CHUNK), jnp.float32),
                block,
                block,
                block,
                block,
                pltpu.VMEM((RING, 2, half, 3 * CHUNK), jnp.bfloat16),
                pltpu.SemaphoreType.DMA((3, steps)),
                pltpu.SemaphoreType.DMA((3, steps)),
                pltpu.SemaphoreType.DMA((PARTS, steps)),
                pltpu.SemaphoreType.DMA((PARTS, steps)),
                pltpu.SemaphoreType.DMA((PARTS, steps)),
                pltpu.SemaphoreType.DMA((PARTS, steps)),
                pltpu.SemaphoreType.DMA((2, steps // 2)),
            ],
            compiler_params=pltpu.CompilerParams(
                collective_id=0, has_side_effects=True, vmem_limit_bytes=48 << 20
            ),
            name="band",
        )(samples)

    return jax.shard_map(
        local, mesh=mesh, in_specs=(P("blk", "feat"),), out_specs=P(None, "blk", "feat"), check_vma=False
    )
```
